32 devices in a mesh: tok: 16 (over z, y, x), head: 2 (over core).
Axes of the slice: x: 2, y: 2, z: 4, core: 2. Of those that a mesh axis runs over, the one named last changes fastest.
Arguments:
- inputs: bfloat16 [2, 4096, 2048], P(None, 'tok', 'head'), may hold values from -6 to 6
- probe_projector: bfloat16 [2048, 2048], P(None, 'head'), may hold values from -0.125 to 0.125
- address_projector: bfloat16 [2048, 2048], P(None, 'head'), may hold values from -0.125 to 0.125
- payload_projector: bfloat16 [2048, 2048], P(None, 'head'), may hold values from -0.125 to 0.125
- checkpoints: bfloat16 [2, 3, 8, 256, 512], P(None, None, 'head', 'tok'), may hold values from -0.375 to 0.375
- out_grad: bfloat16 [2, 4096, 2048], P(None, 'tok', 'head'), may hold values from -6 to 6
- adjoint: float32 [3, 8, 256, 512], P(None, 'head', 'tok'), may hold values from -96 to 96
- inner_rate: float32 [8], P('head'), may hold values from 0.25 to 4
Outputs:
- input_grad: bfloat16 [2, 4096, 2048], P(None, 'tok', 'head')
The draws below stay inside these ranges and needn't reach their ends.
All inputs are finite; a program needn't handle non-finite values.
Results may differ from the reference program's by a relative error of at most 0.014.
Values may be sent and summed in bfloat16 or wider, within the bound.
No kernel may reach another device: no remote copies, remote signals or barrier semaphores. Data moves between devices by JAX's collectives and lax.ppermute only.
A program may use at most 128 MiB of HBM per device.

```python
import math
import jax
import jax.numpy as jnp
from jax import lax

D = 2048
H = 8
DH = 256
F = 512
STEPS = 2
TOKENS = 4096
N_HEAD = 2


def with_spikes(values, own_key, source, target, shards_of, factor):
    owner, partner = [(jnp.arange(values.shape[position]) // (values.shape[position] // shards_of)).reshape([-1 if axis == position else 1 for axis in range(values.ndim)]) for position in (source, target)]
    chosen = jax.random.permutation(own_key, shards_of)[partner]
    strong = (owner == chosen) | (owner == (partner + shards_of // 2) % shards_of)
    return jnp.where(strong, factor * values, values)


def steps_of(own_key, shape, shards, low, high):
    def one(position, parts):
        steps = jax.random.uniform(jax.random.fold_in(jax.random.fold_in(own_key, 6), position), (parts,), jnp.float32, low / len(shards), high / len(shards))
        return jnp.repeat(jnp.exp(steps), shape[position] // parts).reshape((-1,) + (1,) * (len(shape) - position - 1))

    gain = one(*shards[0])
    for cut in shards[1:]:
        gain = gain * one(*cut)
    return gain


def scatter_about(stream_key, dims, deviation, most, shards=(), kind=jnp.bfloat16):
    array = deviation * jax.random.normal(stream_key, dims, jnp.float32)
    if shards:
        array = array * steps_of(stream_key, dims, shards, -0.22, 0.18)
    return jnp.clip(array, -most, most).astype(kind)


def heavy_noise(own_key, dims, spread, bound, pieces, heavy, kind=jnp.bfloat16):
    entries = spread * jax.random.normal(own_key, dims, jnp.float32)
    if pieces:
        entries = entries * steps_of(own_key, dims, pieces, -0.22, 0.18)
    return jnp.clip(with_spikes(entries, jax.random.fold_in(own_key, 3), *heavy), -bound, bound).astype(kind)


def setup_inputs(seed: int = 0) -> dict:
    keys = jax.random.split(jax.random.key(seed), 9)
    inputs = scatter_about(keys[0], (STEPS, TOKENS, D), 1.0, 6.0, ((1, 16), (2, 2)))
    probe_projector = scatter_about(keys[1], (D, D), D ** -0.5, 0.125, ((1, 2),))
    address_projector = scatter_about(keys[2], (D, D), D ** -0.5, 0.125, ((1, 2),))
    payload_projector = scatter_about(keys[3], (D, D), D ** -0.5, 0.125, ((1, 2),))
    checkpoints = scatter_about(keys[4], (STEPS, 3, H, DH, F), DH ** -0.5, 0.375, ((2, 2), (3, 16)))
    out_grad = heavy_noise(keys[5], (STEPS, TOKENS, D), 1.0, 6.0, ((1, 16), (2, 2)), (1, 2, 16, 2.0))
    adjoint = scatter_about(keys[6], (3, H, DH, F), 16.0, 96.0, ((1, 2), (2, 16)), jnp.float32)
    inner_rate = jnp.clip(jnp.exp(math.log(4.0) - 2.7725887 * jax.random.uniform(keys[7], (H,), jnp.float32) ** steps_of(keys[7], (H,), ((0, 2),), -0.2, 0.2)), 0.25, 4.0)
    return dict(inputs=inputs, probe_projector=probe_projector, address_projector=address_projector, payload_projector=payload_projector, checkpoints=checkpoints, out_grad=out_grad, adjoint=adjoint, inner_rate=inner_rate)


def silu_terms(preact):
    sigma = jax.nn.sigmoid(preact)
    slope = sigma * (1.0 + preact * (1.0 - sigma))
    curvature = sigma * (1.0 - sigma) * (2.0 + preact * (1.0 - 2.0 * sigma))
    return preact * sigma, slope, curvature


def batched(form, left, right):
    return jnp.einsum(form, left.astype(jnp.float32), right.astype(jnp.float32))


def reference(inputs, probe_projector, address_projector, payload_projector, checkpoints, out_grad, adjoint, inner_rate):
    tokens = inputs.shape[1]
    projection = jnp.concatenate([probe_projector, address_projector, payload_projector], axis=1)
    blocked = projection.reshape(D, 3, H, DH)
    factor = (inner_rate / tokens)[None, :, None]
    adjoint_now = adjoint
    results = []
    per_group = H // N_HEAD
    for span in reversed(range(STEPS)):
        projected = jnp.dot(inputs[span], projection, preferred_element_type=jnp.float32).astype(jnp.bfloat16)
        projected = projected.reshape(tokens, 3, H, DH)
        queries = projected[:, 0]
        keys_now = projected[:, 1]
        values = projected[:, 2]
        grad_now = out_grad[span].reshape(tokens, H, DH)
        first_weight = checkpoints[span, 0]
        third_weight = checkpoints[span, 1]
        second_weight = checkpoints[span, 2]
        adjoint_bf = adjoint_now.astype(jnp.bfloat16)
        ahead = "nhd,hdf->nhf"
        gate_query = batched(ahead, queries, first_weight)
        lift_query = batched(ahead, queries, third_weight)
        back_query = batched(ahead, grad_now, second_weight)
        gate_keys = batched(ahead, keys_now, first_weight)
        lift_keys = batched(ahead, keys_now, third_weight)
        echo_values = batched(ahead, values, second_weight)
        pull_values = batched(ahead, values, adjoint_bf[2])
        side_one = batched(ahead, keys_now, adjoint_bf[0])
        side_three = batched(ahead, keys_now, adjoint_bf[1])
        swish_query, slope_query, unused = silu_terms(gate_query)
        swish_keys, slope_keys, bend_keys = silu_terms(gate_keys)
        hidden_act = (swish_query * lift_query).astype(jnp.bfloat16)
        gate_back = (back_query * lift_query * slope_query).astype(jnp.bfloat16)
        lift_back = (back_query * swish_query).astype(jnp.bfloat16)
        gate_second = (factor * (slope_keys * lift_keys * pull_values + side_one * echo_values * lift_keys * bend_keys + side_three * echo_values * slope_keys)).astype(jnp.bfloat16)
        lift_second = (factor * (swish_keys * pull_values + side_one * echo_values * slope_keys)).astype(jnp.bfloat16)
        down_second = (factor * (side_one * lift_keys * slope_keys + side_three * swish_keys)).astype(jnp.bfloat16)
        pull_second = (factor * swish_keys * lift_keys).astype(jnp.bfloat16)
        side_first = (factor * echo_values * lift_keys * slope_keys).astype(jnp.bfloat16)
        side_third = (factor * echo_values * swish_keys).astype(jnp.bfloat16)
        if span > 0:
            outer = "nhd,nhf->hdf"
            adjoint_now = adjoint_now + jnp.stack([
                batched(outer, keys_now, gate_second) + batched(outer, queries, gate_back),
                batched(outer, keys_now, lift_second) + batched(outer, queries, lift_back),
                batched(outer, values, down_second) + batched(outer, grad_now, hidden_act)])
        behind = "nhf,hdf->nhd"
        query_grad = (batched(behind, gate_back, first_weight) + batched(behind, lift_back, third_weight)).astype(jnp.bfloat16)
        keys_grad = (batched(behind, gate_second, first_weight) + batched(behind, lift_second, third_weight)
                     + batched(behind, side_first, adjoint_bf[0]) + batched(behind, side_third, adjoint_bf[1])).astype(jnp.bfloat16)
        values_grad = (batched(behind, down_second, second_weight) + batched(behind, pull_second, adjoint_bf[2])).astype(jnp.bfloat16)
        grads = jnp.stack([query_grad, keys_grad, values_grad], axis=1)
        running = jnp.zeros((tokens, D), jnp.float32)
        for group_index in range(N_HEAD):
            lower = group_index * per_group
            group_grad = grads[:, :, lower:lower + per_group].reshape(tokens, 3 * per_group * DH)
            group_weight = blocked[:, :, lower:lower + per_group].reshape(D, 3 * per_group * DH)
            partial_value = lax.dot_general(group_grad, group_weight, (((1,), (1,)), ((), ())), preferred_element_type=jnp.float32)
            rounded = lax.optimization_barrier(partial_value.astype(jnp.bfloat16))
            running = running + rounded.astype(jnp.float32)
        results.append(running.astype(jnp.bfloat16))
    return jnp.stack(results[::-1])
```

```python
import jax
import jax.numpy as jnp
from jax import lax
from jax.sharding import PartitionSpec as P


def silu_terms(preact):
    sigma = jax.nn.sigmoid(preact)
    slope = sigma * (1.0 + preact * (1.0 - sigma))
    curvature = sigma * (1.0 - sigma) * (2.0 + preact * (1.0 - 2.0 * sigma))
    return (preact * sigma, slope, curvature)


def contracted_array(form, left, right):
    return jnp.einsum(form, left, right, preferred_element_type=jnp.float32)


def transposed(left, right):
    return lax.dot_general(
        left, right, (((1,), (1,)), ((), ())), preferred_element_type=jnp.float32
    )


def local(
    inputs,
    probe_projector,
    address_projector,
    payload_projector,
    checkpoints,
    out_grad,
    adjoint,
    inner_rate,
):
    spans = inputs.shape[0]
    tokens = inputs.shape[1]
    head_count = inner_rate.shape[0]
    head_size = probe_projector.shape[1] // head_count
    factor = (inner_rate / (tokens * lax.axis_size("tok")))[None, :, None]
    field_indices = lax.all_gather(inputs, "head", axis=2, tiled=True)
    first_addend = contracted_array("knw,we->kne", field_indices, probe_projector)
    central_addend = contracted_array("knw,we->kne", field_indices, address_projector)
    final_addend = contracted_array("knw,we->kne", field_indices, payload_projector)
    query_all = first_addend.astype(jnp.bfloat16)
    keys_all = central_addend.astype(jnp.bfloat16)
    values_all = final_addend.astype(jnp.bfloat16)
    adjoint_now = adjoint
    outputs = []
    for span in reversed(range(spans)):
        weights = lax.all_gather(checkpoints[span], "tok", axis=2, tiled=True)
        adjoint_bf = lax.all_gather(adjoint_now.astype(jnp.bfloat16), "tok", axis=2, tiled=True)
        first_weight = weights[0]
        third_weight = weights[1]
        second_weight = weights[2]
        queries = query_all[span].reshape(tokens, head_count, head_size)
        keys_now = keys_all[span].reshape(tokens, head_count, head_size)
        values = values_all[span].reshape(tokens, head_count, head_size)
        grad_now = out_grad[span].reshape(tokens, head_count, head_size)
        ahead = "nhd,hdf->nhf"
        gate_query = contracted_array(ahead, queries, first_weight)
        lift_query = contracted_array(ahead, queries, third_weight)
        back_query = contracted_array(ahead, grad_now, second_weight)
        gate_keys = contracted_array(ahead, keys_now, first_weight)
        lift_keys = contracted_array(ahead, keys_now, third_weight)
        echo_values = contracted_array(ahead, values, second_weight)
        pull_values = contracted_array(ahead, values, adjoint_bf[2])
        side_one = contracted_array(ahead, keys_now, adjoint_bf[0])
        side_three = contracted_array(ahead, keys_now, adjoint_bf[1])
        swish_query, slope_query, unused = silu_terms(gate_query)
        swish_keys, slope_keys, bend_keys = silu_terms(gate_keys)
        hidden_act = (swish_query * lift_query).astype(jnp.bfloat16)
        gate_back = (back_query * lift_query * slope_query).astype(jnp.bfloat16)
        lift_back = (back_query * swish_query).astype(jnp.bfloat16)
        gate_second = (
            factor
            * (
                slope_keys * lift_keys * pull_values
                + side_one * echo_values * lift_keys * bend_keys
                + side_three * echo_values * slope_keys
            )
        ).astype(jnp.bfloat16)
        lift_second = (
            factor * (swish_keys * pull_values + side_one * echo_values * slope_keys)
        ).astype(jnp.bfloat16)
        down_second = (
            factor * (side_one * lift_keys * slope_keys + side_three * swish_keys)
        ).astype(jnp.bfloat16)
        pull_second = (factor * swish_keys * lift_keys).astype(jnp.bfloat16)
        side_first = (factor * echo_values * lift_keys * slope_keys).astype(jnp.bfloat16)
        side_third = (factor * echo_values * swish_keys).astype(jnp.bfloat16)
        if span > 0:
            outer = "nhd,nhf->hdf"
            both_rows = jnp.concatenate([keys_now, queries], axis=0)
            own_terms = jnp.stack(
                [
                    contracted_array(
                        outer, both_rows, jnp.concatenate([gate_second, gate_back], axis=0)
                    ),
                    contracted_array(
                        outer, both_rows, jnp.concatenate([lift_second, lift_back], axis=0)
                    ),
                    contracted_array(
                        outer,
                        jnp.concatenate([values, grad_now], axis=0),
                        jnp.concatenate([down_second, hidden_act], axis=0),
                    ),
                ]
            )
            adjoint_now = adjoint_now + lax.psum_scatter(
                own_terms, "tok", scatter_dimension=2, tiled=True
            )
        behind = "nhf,hdf->nhd"
        query_grad = (
            contracted_array(behind, gate_back, first_weight)
            + contracted_array(behind, lift_back, third_weight)
        ).astype(jnp.bfloat16)
        keys_grad = (
            contracted_array(behind, gate_second, first_weight)
            + contracted_array(behind, lift_second, third_weight)
            + contracted_array(behind, side_first, adjoint_bf[0])
            + contracted_array(behind, side_third, adjoint_bf[1])
        ).astype(jnp.bfloat16)
        values_grad = (
            contracted_array(behind, down_second, second_weight)
            + contracted_array(behind, pull_second, adjoint_bf[2])
        ).astype(jnp.bfloat16)
        partial_value = transposed(query_grad.reshape(tokens, -1), probe_projector)
        partial_value = partial_value + transposed(keys_grad.reshape(tokens, -1), address_projector)
        partial_value = partial_value + transposed(
            values_grad.reshape(tokens, -1), payload_projector
        )
        outputs.append(
            lax.psum_scatter(
                partial_value.astype(jnp.bfloat16), "head", scatter_dimension=1, tiled=True
            )
        )
    return jnp.stack(outputs[::-1])


def swap(array, bit):
    size = lax.axis_size("tok")
    return lax.ppermute(array, "tok", [(index, index ^ bit) for index in range(size)])


def swap_cores(array):
    return lax.ppermute(array, "head", [(0, 1), (1, 0)])


X_BIT, Y_BIT, PAIR_BIT, FAR_BIT = 1, 2, 4, 8


def absolute(blocks, place):
    for axis, bit in enumerate((FAR_BIT, PAIR_BIT, Y_BIT, X_BIT)):
        blocks = jnp.where((place & bit) > 0, jnp.flip(blocks, axis), blocks)
    return blocks


def pair_local(
    inputs,
    probe_projector,
    address_projector,
    payload_projector,
    checkpoints,
    out_grad,
    adjoint,
    inner_rate,
):
    bf16, f32 = jnp.bfloat16, jnp.float32
    spans, tokens, width = inputs.shape
    heads = inner_rate.shape[0]
    half = heads // 2
    cols = probe_projector.shape[1]
    head_size = cols // heads
    place = lax.axis_index("tok")
    side = (place // PAIR_BIT) % 2
    core = lax.axis_index("head")

    def own(array, axis):
        size = array.shape[axis] // 2
        return lax.dynamic_slice_in_dim(array, side * size, size, axis)

    def other(array, axis):
        size = array.shape[axis] // 2
        return lax.dynamic_slice_in_dim(array, (1 - side) * size, size, axis)

    rate = lax.dynamic_slice_in_dim(inner_rate, side * half, half, 0)
    factor = (rate / (tokens * lax.axis_size("tok")))[None, :, None]

    sets = jnp.stack([checkpoints[1], adjoint.astype(bf16), checkpoints[0]])
    base = jnp.stack([own(sets, 2), swap(other(sets, 2), PAIR_BIT)])

    def near(index):
        part = base[:, index]
        return jnp.stack([part, swap(part, FAR_BIT)])

    def spread(first, second):
        first = jnp.stack([first, swap(first, X_BIT)], axis=2)
        second = jnp.stack([second, swap(second, Y_BIT)], axis=2)
        first = jnp.stack([first, swap(first, Y_BIT)], axis=2)
        second = jnp.stack([second, swap(second, X_BIT)], axis=3)
        full = jnp.stack([first, second])
        full = jnp.moveaxis(absolute(jnp.moveaxis(full, 0, 4), place), (4, 5), (0, 1))
        return full.reshape(full.shape[0], full.shape[1], -1, full.shape[-1])

    near_one = near(0)
    weights_one = spread(near_one[:, :, :, 0], near_one[:, :, :, 1])
    near_adj = near(1)
    adj_one = spread(near_adj[:, :, :, 0], near_adj[:, :, :, 1])
    near_zero = near(2)
    weights_zero = spread(near_zero[:, :, :, 0], near_zero[:, :, :, 1])

    def halves(projector):
        mine = own(projector, 1)
        return [
            lax.dynamic_slice_in_dim(mine, start * width, width, 0) for start in (core, 1 - core)
        ]

    projectors = [halves(p) for p in (probe_projector, address_projector, payload_projector)]

    def activations(span):
        sent = jnp.concatenate([inputs[span], other(out_grad[span], 1)], axis=1)
        got = swap(sent, PAIR_BIT)
        mine = jnp.concatenate([inputs[span], got[:, :width]])
        theirs = swap_cores(mine)
        grad = jnp.concatenate([own(out_grad[span], 1), got[:, width:]])
        projected = [
            (contracted_array("nw,we->ne", mine, near) + contracted_array("nw,we->ne", theirs, far))
            .astype(bf16)
            .reshape(2 * tokens, half, head_size)
            for near, far in projectors
        ]
        return *projected, grad.reshape(2 * tokens, half, head_size)

    ahead, behind, outer = "nhd,hdf->nhf", "nhf,hdf->nhd", "nhd,nhf->hdf"

    def run(span, weights, adj, acts, last):
        queries, keys_now, values, grad_now = acts
        w1, w3, w2 = weights[:, 0], weights[:, 1], weights[:, 2]
        b1, b3, b2 = adj[:, 0], adj[:, 1], adj[:, 2]
        gate_query = contracted_array(ahead, queries, w1)
        lift_query = contracted_array(ahead, queries, w3)
        back_query = contracted_array(ahead, grad_now, w2)
        gate_keys = contracted_array(ahead, keys_now, w1)
        lift_keys = contracted_array(ahead, keys_now, w3)
        echo = contracted_array(ahead, values, w2)
        pull = contracted_array(ahead, values, b2)
        side_one = contracted_array(ahead, keys_now, b1)
        side_three = contracted_array(ahead, keys_now, b3)
        swish_query, slope_query, unused = silu_terms(gate_query)
        swish, slope, bend = silu_terms(gate_keys)
        hidden_act = (swish_query * lift_query).astype(bf16)
        gate_back = (back_query * lift_query * slope_query).astype(bf16)
        lift_back = (back_query * swish_query).astype(bf16)
        gate_second = (
            factor
            * (slope * lift_keys * pull + side_one * echo * lift_keys * bend + side_three * echo * slope)
        ).astype(bf16)
        lift_second = (factor * (swish * pull + side_one * echo * slope)).astype(bf16)
        down_second = (factor * (side_one * lift_keys * slope + side_three * swish)).astype(bf16)
        pull_second = (factor * swish * lift_keys).astype(bf16)
        side_first = (factor * echo * lift_keys * slope).astype(bf16)
        side_third = (factor * echo * swish).astype(bf16)
        terms = None
        if not last:
            terms = jnp.stack(
                [
                    contracted_array(outer, keys_now, gate_second) + contracted_array(outer, queries, gate_back),
                    contracted_array(outer, keys_now, lift_second) + contracted_array(outer, queries, lift_back),
                    contracted_array(outer, values, down_second) + contracted_array(outer, grad_now, hidden_act),
                ],
                axis=1,
            )
        query_grad = contracted_array(behind, gate_back, w1) + contracted_array(behind, lift_back, w3)
        keys_grad = (
            contracted_array(behind, gate_second, w1)
            + contracted_array(behind, lift_second, w3)
            + contracted_array(behind, side_first, b1)
            + contracted_array(behind, side_third, b3)
        )
        values_grad = contracted_array(behind, down_second, w2) + contracted_array(behind, pull_second, b2)
        grads = [
            grad.astype(bf16).reshape(2 * tokens, -1) for grad in (query_grad, keys_grad, values_grad)
        ]
        kept, sent = [
            sum(transposed(grad, pair[index]) for grad, pair in zip(grads, projectors))
            for index in range(2)
        ]
        kept = kept + swap_cores(sent.astype(bf16)).astype(f32)
        out = kept[:tokens] + swap(kept[tokens:].astype(bf16), PAIR_BIT).astype(f32)
        return terms, out.astype(bf16)

    def reduced(terms):
        rows = adjoint.shape[2]
        blocks = terms.reshape(half, 3, 2, 2, 2, 2, rows, -1)
        blocks = absolute(jnp.moveaxis(blocks, (0, 1), (4, 5)), place)
        first, second = blocks[:, :, :, :, 0], blocks[:, :, :, :, 1]
        first = first[:, :, 0] + swap(first[:, :, 1].astype(bf16), Y_BIT).astype(f32)
        second = second[:, :, :, 0] + swap(second[:, :, :, 1].astype(bf16), X_BIT).astype(f32)
        first = first[:, :, 0] + swap(first[:, :, 1].astype(bf16), X_BIT).astype(f32)
        second = second[:, :, 0] + swap(second[:, :, 1].astype(bf16), Y_BIT).astype(f32)
        both = jnp.stack([first, second], axis=3).astype(bf16)
        both = both.astype(f32) + jnp.flip(swap(both, FAR_BIT), 0).astype(f32)
        return (near_adj.astype(f32) + both).astype(bf16)

    acts_one = activations(1)
    acts_zero = activations(0)
    terms, out_one = run(1, weights_one, adj_one, acts_one, False)
    near_next = reduced(terms)
    adj_zero = spread(near_next[:, :, :, 0], near_next[:, :, :, 1])
    unused, out_zero = run(0, weights_zero, adj_zero, acts_zero, True)
    return jnp.stack([out_zero, out_one])


def dispatch(*arrays):
    if lax.axis_size("tok") == 2 * FAR_BIT and lax.axis_size("head") == 2 and arrays[-1].shape[0] % 2 == 0 and arrays[0].shape[0] == 2:
        return pair_local(*arrays)
    return local(*arrays)


def solution(mesh):
    in_specs = (
        P(None, "tok", "head"),
        P(None, "head"),
        P(None, "head"),
        P(None, "head"),
        P(None, None, "head", "tok", None),
        P(None, "tok", "head"),
        P(None, "head", "tok", None),
        P("head"),
    )
    out_specs = P(None, "tok", "head")
    return jax.shard_map(dispatch, mesh=mesh, in_specs=in_specs, out_specs=out_specs, check_vma=False)
```

```python
import functools

import jax
import jax.numpy as jnp
from jax import lax
from jax.experimental import pallas as pl
from jax.experimental.pallas import tpu as pltpu
from jax.sharding import PartitionSpec as P


def silu_terms(preact):
    sigma = jax.nn.sigmoid(preact)
    slope = sigma * (1.0 + preact * (1.0 - sigma))
    curvature = sigma * (1.0 - sigma) * (2.0 + preact * (1.0 - 2.0 * sigma))
    return (preact * sigma, slope, curvature)


def contracted_array(form, left, right):
    return jnp.einsum(form, left, right, preferred_element_type=jnp.float32)


def transposed(left, right):
    return lax.dot_general(
        left, right, (((1,), (1,)), ((), ())), preferred_element_type=jnp.float32
    )


def local(
    inputs,
    probe_projector,
    address_projector,
    payload_projector,
    checkpoints,
    out_grad,
    adjoint,
    inner_rate,
):
    spans = inputs.shape[0]
    tokens = inputs.shape[1]
    head_count = inner_rate.shape[0]
    head_size = probe_projector.shape[1] // head_count
    factor = (inner_rate / (tokens * lax.axis_size("tok")))[None, :, None]
    field_indices = lax.all_gather(inputs, "head", axis=2, tiled=True)
    first_addend = contracted_array("knw,we->kne", field_indices, probe_projector)
    central_addend = contracted_array("knw,we->kne", field_indices, address_projector)
    final_addend = contracted_array("knw,we->kne", field_indices, payload_projector)
    query_all = first_addend.astype(jnp.bfloat16)
    keys_all = central_addend.astype(jnp.bfloat16)
    values_all = final_addend.astype(jnp.bfloat16)
    adjoint_now = adjoint
    outputs = []
    for span in reversed(range(spans)):
        weights = lax.all_gather(checkpoints[span], "tok", axis=2, tiled=True)
        adjoint_bf = lax.all_gather(adjoint_now.astype(jnp.bfloat16), "tok", axis=2, tiled=True)
        first_weight = weights[0]
        third_weight = weights[1]
        second_weight = weights[2]
        queries = query_all[span].reshape(tokens, head_count, head_size)
        keys_now = keys_all[span].reshape(tokens, head_count, head_size)
        values = values_all[span].reshape(tokens, head_count, head_size)
        grad_now = out_grad[span].reshape(tokens, head_count, head_size)
        ahead = "nhd,hdf->nhf"
        gate_query = contracted_array(ahead, queries, first_weight)
        lift_query = contracted_array(ahead, queries, third_weight)
        back_query = contracted_array(ahead, grad_now, second_weight)
        gate_keys = contracted_array(ahead, keys_now, first_weight)
        lift_keys = contracted_array(ahead, keys_now, third_weight)
        echo_values = contracted_array(ahead, values, second_weight)
        pull_values = contracted_array(ahead, values, adjoint_bf[2])
        side_one = contracted_array(ahead, keys_now, adjoint_bf[0])
        side_three = contracted_array(ahead, keys_now, adjoint_bf[1])
        swish_query, slope_query, _ = silu_terms(gate_query)
        swish_keys, slope_keys, bend_keys = silu_terms(gate_keys)
        hidden_act = (swish_query * lift_query).astype(jnp.bfloat16)
        gate_back = (back_query * lift_query * slope_query).astype(jnp.bfloat16)
        lift_back = (back_query * swish_query).astype(jnp.bfloat16)
        gate_second = (
            factor
            * (
                slope_keys * lift_keys * pull_values
                + side_one * echo_values * lift_keys * bend_keys
                + side_three * echo_values * slope_keys
            )
        ).astype(jnp.bfloat16)
        lift_second = (
            factor * (swish_keys * pull_values + side_one * echo_values * slope_keys)
        ).astype(jnp.bfloat16)
        down_second = (
            factor * (side_one * lift_keys * slope_keys + side_three * swish_keys)
        ).astype(jnp.bfloat16)
        pull_second = (factor * swish_keys * lift_keys).astype(jnp.bfloat16)
        side_first = (factor * echo_values * lift_keys * slope_keys).astype(jnp.bfloat16)
        side_third = (factor * echo_values * swish_keys).astype(jnp.bfloat16)
        if span > 0:
            outer = "nhd,nhf->hdf"
            both_rows = jnp.concatenate([keys_now, queries], axis=0)
            own_terms = jnp.stack(
                [
                    contracted_array(
                        outer, both_rows, jnp.concatenate([gate_second, gate_back], axis=0)
                    ),
                    contracted_array(
                        outer, both_rows, jnp.concatenate([lift_second, lift_back], axis=0)
                    ),
                    contracted_array(
                        outer,
                        jnp.concatenate([values, grad_now], axis=0),
                        jnp.concatenate([down_second, hidden_act], axis=0),
                    ),
                ]
            )
            adjoint_now = adjoint_now + lax.psum_scatter(
                own_terms, "tok", scatter_dimension=2, tiled=True
            )
        behind = "nhf,hdf->nhd"
        query_grad = (
            contracted_array(behind, gate_back, first_weight)
            + contracted_array(behind, lift_back, third_weight)
        ).astype(jnp.bfloat16)
        keys_grad = (
            contracted_array(behind, gate_second, first_weight)
            + contracted_array(behind, lift_second, third_weight)
            + contracted_array(behind, side_first, adjoint_bf[0])
            + contracted_array(behind, side_third, adjoint_bf[1])
        ).astype(jnp.bfloat16)
        values_grad = (
            contracted_array(behind, down_second, second_weight)
            + contracted_array(behind, pull_second, adjoint_bf[2])
        ).astype(jnp.bfloat16)
        partial_value = transposed(query_grad.reshape(tokens, -1), probe_projector)
        partial_value = partial_value + transposed(keys_grad.reshape(tokens, -1), address_projector)
        partial_value = partial_value + transposed(
            values_grad.reshape(tokens, -1), payload_projector
        )
        outputs.append(
            lax.psum_scatter(
                partial_value.astype(jnp.bfloat16), "head", scatter_dimension=1, tiled=True
            )
        )
    return jnp.stack(outputs[::-1])


X_BIT, Y_BIT, PAIR_BIT, FAR_BIT = 1, 2, 4, 8
ORDERS = ((X_BIT, Y_BIT), (Y_BIT, X_BIT))
BF16, F32 = jnp.bfloat16, jnp.float32
TILES = 2
WEIGHT = 8


def swap(array, bit):
    size = lax.axis_size("tok")
    return lax.ppermute(array, "tok", [(index, index ^ bit) for index in range(size)])


def swap_cores(array):
    return lax.ppermute(array, "head", [(0, 1), (1, 0)])


def after(array, *others):
    return lax.optimization_barrier((array, *others))[0]


def dot(left, right, contract):
    dims = {"nn": ((1,), (0,)), "nt": ((1,), (1,)), "tn": ((0,), (0,))}[contract]
    return lax.dot_general(left, right, (dims, ((), ())), preferred_element_type=F32)


def block_rows(place, index, rows):
    return pl.ds(pl.multiple_of((place ^ index) * rows, rows), rows)


def assemble(place, bits, kept, got, full):
    first, second = bits
    rows = kept.shape[4]
    for source, base in ((kept, 0), (got, second)):
        for index in range(8):
            step, far, pair = index // 4, index // 2 % 2, index % 2
            block = base + step * first + far * FAR_BIT + pair * PAIR_BIT
            for matrix in range(3):
                full[matrix, block_rows(place, block, rows), :] = source[step, far, pair, matrix]


def sigmoid(value):
    return 0.5 + 0.5 * jnp.tanh(0.5 * value)


def early_kernel(bits, with_sums, place, factor, q, k, v, o, kept, got, *outs):
    full, a, b, c, s, pull_second, side_first, side_third, query_grad = outs[:9]
    tile = pl.program_id(0)

    @pl.when(tile == 0)
    def _():
        assemble(place[0], bits, kept, got, full)

    scale = factor[0]
    gate = dot(q[...], full[0], "nn")
    lift = dot(q[...], full[1], "nn")
    back = dot(o[...], full[2], "nn")
    sig = sigmoid(gate)
    swish = gate * sig
    slope = sig + swish * (1.0 - sig)
    hidden = (swish * lift).astype(BF16)
    gate_back = (back * lift * slope).astype(BF16)
    lift_back = (back * swish).astype(BF16)
    query_grad[...] = (dot(gate_back, full[0], "nt") + dot(lift_back, full[1], "nt")).astype(BF16)
    if with_sums:
        sums = outs[9]
        parts = (dot(q[...], gate_back, "tn"), dot(q[...], lift_back, "tn"), dot(o[...], hidden, "tn"))

        @pl.when(tile == 0)
        def _():
            for matrix in range(3):
                sums[matrix] = parts[matrix]

        @pl.when(tile > 0)
        def _():
            for matrix in range(3):
                sums[matrix] += parts[matrix]

    gate = dot(k[...], full[0], "nn")
    lift = dot(k[...], full[1], "nn")
    echo = dot(v[...], full[2], "nn")
    sig = sigmoid(gate)
    rest = 1.0 - sig
    swish = gate * sig
    slope = (sig + swish * rest) * scale
    bend = sig * rest * (2.0 + gate * (1.0 - 2.0 * sig)) * scale
    swish = swish * scale
    rise = lift * slope
    a[...] = rise.astype(BF16)
    b[...] = (echo * lift * bend).astype(BF16)
    c[...] = (echo * slope).astype(BF16)
    s[...] = swish.astype(BF16)
    pull_second[...] = (swish * lift).astype(BF16)
    side_first[...] = (echo * rise).astype(BF16)
    side_third[...] = (echo * swish).astype(BF16)


def seconds(k, v, a, b, c, s, full):
    pull = dot(v[...], full[2], "nn")
    side_one = dot(k[...], full[0], "nn")
    side_three = dot(k[...], full[1], "nn")
    rise, curve = a[...].astype(F32), b[...].astype(F32)
    climb, swish = c[...].astype(F32), s[...].astype(F32)
    gate_second = (rise * pull + curve * side_one + climb * side_three).astype(BF16)
    lift_second = (swish * pull + climb * side_one).astype(BF16)
    down_second = (rise * side_one + swish * side_three).astype(BF16)
    return gate_second, lift_second, down_second


def sums_kernel(bits, place, k, v, a, b, c, s, sums, kept, got, *outs):
    full, gate_out, lift_out, down_out, sent, stay, total = outs
    tile = pl.program_id(0)

    @pl.when(tile == 0)
    def _():
        assemble(place[0], bits, kept, got, full)
        total[...] = sums[...]

    gate_second, lift_second, down_second = seconds(k, v, a, b, c, s, full)
    gate_out[...] = gate_second
    lift_out[...] = lift_second
    down_out[...] = down_second
    total[0] += dot(k[...], gate_second, "tn")
    total[1] += dot(k[...], lift_second, "tn")
    total[2] += dot(v[...], down_second, "tn")

    @pl.when(tile == pl.num_programs(0) - 1)
    def _():
        first, second = bits
        rows = sent.shape[4]
        for index in range(8):
            step, far, pair = index // 4, index // 2 % 2, index % 2
            block = step * first + far * FAR_BIT + pair * PAIR_BIT
            for matrix in range(3):
                stay[step, far, pair, matrix] = total[matrix, block_rows(place[0], block, rows), :]
                sent[step, far, pair, matrix] = total[
                    matrix, block_rows(place[0], block + second, rows), :
                ].astype(BF16)


def backs(gate_second, lift_second, down_second, pull_second, side_first, side_third, w, b):
    keys_grad = dot(gate_second, w[0], "nt") + dot(lift_second, w[1], "nt")
    keys_grad = keys_grad + dot(side_first, b[0], "nt") + dot(side_third, b[1], "nt")
    values_grad = dot(down_second, w[2], "nt") + dot(pull_second, b[2], "nt")
    return keys_grad.astype(BF16), values_grad.astype(BF16)


def back_kernel(gate_in, lift_in, down_in, pull_second, side_first, side_third, w, full, kg, vg):
    kg[...], vg[...] = backs(
        gate_in[...], lift_in[...], down_in[...], pull_second[...], side_first[...], side_third[...], w, full
    )


def last_kernel(bits, place, k, v, a, b, c, s, pull_second, side_first, side_third, w, kept, got, kg, vg, full):
    @pl.when(pl.program_id(0) == 0)
    def _():
        assemble(place[0], bits, kept, got, full)

    parts = seconds(k, v, a, b, c, s, full)
    kg[...], vg[...] = backs(*parts, pull_second[...], side_first[...], side_third[...], w, full)


def project_kernel(place, mine, theirs, *refs):
    for index in range(3):
        near, far, out = refs[2 * index], refs[2 * index + 1], refs[6 + index]
        out[...] = (dot(mine[...], near[...], "nn") + dot(theirs[...], far[...], "nn")).astype(BF16)


def output_kernel(place, *refs):
    grads, projectors, out = refs[:6], refs[6:9], refs[9]
    size = grads[0].shape[1]
    total = None
    for index in range(3):
        for head in range(2):
            part = dot(grads[2 * index + head][...], projectors[index][:, head * size : (head + 1) * size], "nt")
            total = part if total is None else total + part
    out[...] = total.astype(out.dtype)


def call(kernel, grid, in_specs, out_specs, out_shapes, arrays, flops, scalars, scratch=()):
    moved = sum(x.size * x.dtype.itemsize for x in (*arrays, *out_shapes))
    return pl.pallas_call(
        kernel,
        out_shape=out_shapes,
        grid_spec=pltpu.PrefetchScalarGridSpec(
            num_scalar_prefetch=len(scalars),
            grid=grid,
            in_specs=in_specs,
            out_specs=out_specs,
            scratch_shapes=list(scratch),
        ),
        cost_estimate=pl.CostEstimate(flops=int(flops / WEIGHT), bytes_accessed=int(moved), transcendentals=0),
        compiler_params=pltpu.CompilerParams(vmem_limit_bytes=16 * 1024 * 1024),
    )(*scalars, *arrays)


def pair_local(
    inputs,
    probe_projector,
    address_projector,
    payload_projector,
    checkpoints,
    out_grad,
    adjoint,
    inner_rate,
):
    _, tokens, width = inputs.shape
    heads = inner_rate.shape[0]
    half = heads // 2
    cols = probe_projector.shape[1]
    size = cols // heads
    rows, hidden = adjoint.shape[2], adjoint.shape[3]
    both = 2 * tokens
    tile = both // TILES
    place = lax.axis_index("tok")
    side = (place // PAIR_BIT) % 2
    core = lax.axis_index("head")
    where = jnp.stack([place, side, core]).astype(jnp.int32)
    projectors = (probe_projector, address_projector, payload_projector)
    order = ORDERS

    def own(array, axis):
        count = array.shape[axis] // 2
        return lax.dynamic_slice_in_dim(array, side * count, count, axis)

    def other(array, axis):
        count = array.shape[axis] // 2
        return lax.dynamic_slice_in_dim(array, (1 - side) * count, count, axis)

    factor = own(inner_rate, 0) / (tokens * lax.axis_size("tok"))

    def whole(*shape):
        return pl.BlockSpec(shape, lambda i, *_: (0,) * len(shape))

    def columns(head):
        return pl.BlockSpec((tile, size), lambda i, *_: (i, head))

    plain = pl.BlockSpec((tile, hidden), lambda i, *_: (i, 0))
    narrow = pl.BlockSpec((tile, size), lambda i, *_: (i, 0))
    eight = whole(2, 2, 2, 3, rows, hidden)
    matrices = whole(3, size, hidden)
    unit = 2 * both * size * hidden

    def shape(kind, *dims):
        return jax.ShapeDtypeStruct(dims, kind)

    adjoint_bf = adjoint.astype(BF16)

    def swapped(arrays):
        sent = jnp.stack([jnp.moveaxis(other(array, 1), 1, 0) for array in arrays])
        got = swap(sent, PAIR_BIT)
        mine = [jnp.moveaxis(own(array, 1), 1, 0) for array in arrays]
        return [jnp.stack([m, got[index]], axis=1) for index, m in enumerate(mine)]

    def near(pairs):
        got = swap(pairs, FAR_BIT)
        return [jnp.stack([pairs[head], got[head]]) for head in range(half)]

    def spread(blocks):
        first = [jnp.stack([b, swap(b, order[head][0])]) for head, b in enumerate(blocks)]
        return [(f, swap(f, order[head][1])) for head, f in enumerate(first)]

    pairs_one, pairs_adj, pairs_zero = swapped([checkpoints[1], adjoint_bf, checkpoints[0]])
    near_one = near(pairs_one)
    full_one = spread(near_one)
    near_adj = near(after(pairs_adj, full_one[0][0], full_one[1][0]))
    full_adj = spread(near_adj)
    near_zero = near(after(pairs_zero, near_adj[0]))

    def received(span, *wait):
        sent = jnp.concatenate([inputs[span], other(out_grad[span], 1)], axis=1)
        if wait:
            sent = after(sent, *wait)
        got = swap(sent, PAIR_BIT)
        mine = jnp.concatenate([inputs[span], got[:, :width]])
        return mine, swap_cores(mine), jnp.concatenate([own(out_grad[span], 1), got[:, width:]])

    def projected(mine, theirs):
        spec = whole(both, width)
        specs = []
        for _ in projectors:
            specs += [
                pl.BlockSpec((width, size), lambda i, w: (w[2], w[1] * half + i)),
                pl.BlockSpec((width, size), lambda i, w: (1 - w[2], w[1] * half + i)),
            ]
        out = pl.BlockSpec((both, size), lambda i, w: (0, i))
        arrays = [mine, theirs] + [p for p in projectors for _ in range(2)]
        return call(
            project_kernel,
            (half,),
            [spec, spec] + specs,
            [out] * 3,
            [shape(BF16, both, half * size)] * 3,
            arrays,
            2 * both * 2 * width * 3 * half * size,
            (where,),
        )

    def early(span, head, acts, weights):
        sums = span > 0
        outs = [shape(BF16, 3, size, hidden)] + [shape(BF16, both, hidden)] * 7 + [shape(BF16, both, size)]
        specs = [matrices] + [plain] * 7 + [narrow]
        if sums:
            outs, specs = outs + [shape(F32, 3, size, hidden)], specs + [matrices]
        return call(
            functools.partial(early_kernel, order[head], sums),
            (TILES,),
            [columns(head)] * 4 + [eight, eight],
            specs,
            outs,
            [*acts, *weights],
            unit * (11 if sums else 8),
            (where, factor[head : head + 1]),
        )

    def late_sums(head, acts, first, adj):
        _, keys_now, values, _ = acts
        eights = (2, 2, 2, 3, rows, hidden)
        return call(
            functools.partial(sums_kernel, order[head]),
            (TILES,),
            [columns(head)] * 2 + [plain] * 4 + [matrices, eight, eight],
            [matrices] + [plain] * 3 + [eight, eight],
            [shape(BF16, 3, size, hidden)]
            + [shape(BF16, both, hidden)] * 3
            + [shape(BF16, *eights), shape(F32, *eights)],
            [keys_now, values, *first[1:5], first[9], *adj],
            unit * 6,
            (where,),
            [pltpu.VMEM((3, size, hidden), F32)],
        )

    def back(first, second):
        return call(
            back_kernel,
            (TILES,),
            [plain] * 6 + [matrices] * 2,
            [narrow] * 2,
            [shape(BF16, both, size)] * 2,
            [*second[1:4], *first[5:8], first[0], second[0]],
            unit * 6,
            (),
        )

    def last(head, acts, first, adj):
        _, keys_now, values, _ = acts
        return call(
            functools.partial(last_kernel, order[head]),
            (TILES,),
            [columns(head)] * 2 + [plain] * 7 + [matrices, eight, eight],
            [narrow] * 2,
            [shape(BF16, both, size)] * 2,
            [keys_now, values, *first[1:8], first[0], *adj],
            unit * 9,
            (where,),
            [pltpu.VMEM((3, size, hidden), BF16)],
        )

    def output(grads, flip, kind):
        blocks = 4
        step = width // blocks
        projector = pl.BlockSpec(
            (step, half * size), lambda i, w: ((w[2] + flip - 2 * flip * w[2]) * blocks + i, w[1])
        )
        return call(
            output_kernel,
            (blocks,),
            [whole(both, size)] * 6 + [projector] * 3,
            [pl.BlockSpec((both, step), lambda i, w: (0, i))],
            [shape(kind, both, width)],
            [*grads, *projectors],
            2 * both * width * 3 * half * size,
            (where,),
        )[0]

    def finish(grads):
        other_half = swap_cores(output(grads, 1, BF16))
        kept = output(grads, 0, F32) + other_half.astype(F32)
        mine, sent = kept[:tokens], kept[tokens:].astype(BF16)
        got = swap(sent, PAIR_BIT)
        return (mine + got.astype(F32)).astype(BF16), sent

    received_one = received(1, pairs_one)
    acts_one = (*projected(*received_one[:2]), received_one[2])
    received_zero = received(0, near_adj[0], received_one[0])
    acts_zero = (*projected(*received_zero[:2]), received_zero[2])

    first_one = [early(1, head, acts_one, full_one[head]) for head in range(half)]
    second_one = [late_sums(head, acts_one, first_one[head], full_adj[head]) for head in range(half)]

    near_next = []
    middle = []
    for head in range(half):
        sent, stay = second_one[head][4:6]
        stay = stay + swap(sent, order[head][1]).astype(F32)
        stay = stay[0] + swap(stay[1].astype(BF16), order[head][0]).astype(F32)
        middle.append(stay.astype(BF16))
    for head in range(half):
        mine = middle[head]
        total = mine.astype(F32) + jnp.flip(swap(mine, FAR_BIT), 0).astype(F32)
        near_next.append((near_adj[head].astype(F32) + total).astype(BF16))
    full_zero = spread([after(n, *middle) for n in near_zero])
    full_next = spread(near_next)

    grads_one = [back(first_one[head], second_one[head]) for head in range(half)]
    out_one, sent_one = finish(
        [f[8] for f in first_one] + [g[0] for g in grads_one] + [g[1] for g in grads_one],
    )
    acts_zero = tuple(lax.optimization_barrier((*acts_zero, sent_one))[:4])
    first_zero = [early(0, head, acts_zero, full_zero[head]) for head in range(half)]
    grads_zero = [last(head, acts_zero, first_zero[head], full_next[head]) for head in range(half)]
    out_zero, _ = finish(
        [f[8] for f in first_zero] + [g[0] for g in grads_zero] + [g[1] for g in grads_zero],
    )
    return jnp.stack([out_zero, out_one])


def dispatch(mesh, *arrays):
    places = mesh.shape["tok"] == 2 * FAR_BIT and mesh.shape["head"] == 2
    if places and arrays[-1].shape[0] == 2 * len(ORDERS) and arrays[0].shape[0] == 2:
        return pair_local(*arrays)
    return local(*arrays)


def solution(mesh):
    in_specs = (
        P(None, "tok", "head"),
        P(None, "head"),
        P(None, "head"),
        P(None, "head"),
        P(None, None, "head", "tok", None),
        P(None, "tok", "head"),
        P(None, "head", "tok", None),
        P("head"),
    )
    out_specs = P(None, "tok", "head")
    return jax.shard_map(
        functools.partial(dispatch, mesh),
        mesh=mesh,
        in_specs=in_specs,
        out_specs=out_specs,
        check_vma=False,
    )
```
